32 devices in a mesh: rep: 2 (over core), tab: 16 (over z, y, x).
Axes of the slice: x: 2, y: 2, z: 4, core: 2. Of those that a mesh axis runs over, the one named last changes fastest.
Arguments:
- grad_out: bfloat16 [8192, 16, 128], P(('rep', 'tab')), may hold values from -1.5 to 1.5
- indices: int32 [16, 8192], P('tab', 'rep'), may hold values from 0 to 1023
- projections: bfloat16 [16, 128, 128], P('tab'), may hold values from -0.75 to 0.75
- widths: int32 [16], replicated, may hold values from 16 to 128
- hot_ids: int32 [16, 32], P('tab'), may hold values from 0 to 1023, as said below
Outputs:
- cold_grad: float32 [2, 16, 1024, 128], P('rep', 'tab')
- hot_grad: float32 [16, 32, 128], P('tab', 'rep')
The draws below stay inside these ranges and needn't reach their ends.
Inputs may be any that keep to these rules, and one draw needn't show every extreme that they name: `hot_ids`: the 32 hot rows of one table are distinct.
All inputs are finite; a program needn't handle non-finite values.
Results may differ from the reference program's by a relative error of at most 0.005.
Values may be sent and summed in bfloat16 or wider, within the bound.
No kernel may reach another device: no remote copies, remote signals or barrier semaphores. Data moves between devices by JAX's collectives and lax.ppermute only.
A program may use at most 128 MiB of HBM per device.

```python
import jax
import jax.numpy as jnp
from jax import lax

BASE = 128
ROWS = 1024
HOT = 32
NT = 16
HALF = 4096
BATCH = 8192
N_REP = 2


def shared_hot(key):
    table_keys = jax.random.split(jax.random.fold_in(key, 7), NT)
    return jax.vmap(lambda table_key: jax.random.permutation(table_key, ROWS)[:HOT])(table_keys).astype(jnp.int32)


def draw_hot_ids(key, part):
    return shared_hot(key)


def draw_indices(key, part):
    hot_rows = shared_hot(key)
    pick_key = jax.random.fold_in(key, 11)
    cold_key = jax.random.fold_in(key, 13)
    use_key = jax.random.fold_in(key, 17)
    pick = jax.random.randint(pick_key, (NT, BATCH), 0, HOT, dtype=jnp.int32)
    drawn = jax.random.randint(cold_key, (NT, BATCH), 0, ROWS, dtype=jnp.int32)
    use_hot = jax.random.randint(use_key, (NT, BATCH), 0, 8, dtype=jnp.int32) == 0
    chosen = jnp.take_along_axis(hot_rows, pick, axis=1)
    return jnp.where(use_hot, chosen, drawn).astype(jnp.int32)


def plant(result, stream_key, low, top_value):
    dims = result.shape
    place = [jax.random.randint(jax.random.fold_in(stream_key, axis), (), 0, dims[axis]) for axis in range(len(dims))]
    result = result.at[tuple(place)].set(low)
    longest = dims.index(max(dims))
    place[longest] = (place[longest] + 1) % dims[longest]
    return result.at[tuple(place)].set(top_value)


def levels(own_key, extent, cuts, smallest, largest):
    def one(dim, shards_of):
        draws = jax.random.uniform(jax.random.fold_in(jax.random.fold_in(own_key, 6), dim), (shards_of,), jnp.float32, smallest / len(cuts), largest / len(cuts))
        return jnp.repeat(jnp.exp(draws), extent[dim] // shards_of).reshape((-1,) + (1,) * (len(extent) - dim - 1))

    level = one(*cuts[0])
    for cut in cuts[1:]:
        level = level * one(*cut)
    return level


def gaussian(key, shape, scale, reach, shards=(), kind=jnp.bfloat16):
    level = levels(key, shape, shards, -0.22, 0.18) if shards else 1.0
    drawn = jax.random.normal(key, shape, jnp.float32) * scale * level
    return jnp.minimum(jnp.maximum(drawn, -reach), reach).astype(kind)


def setup_inputs(seed: int = 0) -> dict:
    streams_of = jax.random.split(jax.random.key(seed), 6)
    grad_out = gaussian(streams_of[0], (BATCH, NT, BASE), 0.25, 1.5, ((0, 32),))
    indices = draw_indices(jax.random.fold_in(streams_of[5], 71), 0)
    projections = gaussian(streams_of[2], (NT, BASE, BASE), (BASE // 2) ** -0.5, 0.75, ((0, 16),))
    widths = plant(jax.random.randint(streams_of[3], (NT,), BASE // 8, BASE + 1), jax.random.fold_in(streams_of[3], 1), BASE // 8, BASE).astype(jnp.int32)
    hot_ids = draw_hot_ids(jax.random.fold_in(streams_of[5], 71), 0)
    return {"grad_out": grad_out, "indices": indices, "projections": projections, "widths": widths, "hot_ids": hot_ids}


def reference(grad_out, indices, projections, widths, hot_ids):
    columns = jnp.arange(BASE, dtype=jnp.int32)
    all_rows = jnp.arange(ROWS, dtype=jnp.int32)

    def one_table(packed):
        table, lookups, project_w, width, hot_rows = packed
        grads = lax.dynamic_index_in_dim(grad_out, table, 1, keepdims=False)
        full_proj = jnp.dot(grads, project_w, preferred_element_type=jnp.float32)
        projected = jnp.where(columns[None, :] < width, full_proj, 0.0).astype(jnp.bfloat16)
        halves_proj = projected.reshape(N_REP, HALF, BASE)
        halves_rows = lookups.reshape(N_REP, HALF)
        row_grads = jnp.stack([jax.ops.segment_sum(halves_proj[half].astype(jnp.float32), halves_rows[half], num_segments=ROWS) for half in range(N_REP)])
        picked = row_grads[:, hot_rows, :]
        hot_sum = picked[0] + picked[1]
        is_hot = jnp.any(hot_rows[:, None] == all_rows[None, :], axis=0)
        cold_rows = jnp.where(is_hot[None, :, None], jnp.float32(0.0), row_grads)
        return cold_rows, hot_sum

    tables = jnp.arange(NT, dtype=jnp.int32)
    cold_all, hot_all = lax.map(one_table, (tables, indices, projections, widths, hot_ids))
    return jnp.swapaxes(cold_all, 0, 1), hot_all
```

```python
import math

import jax
import jax.numpy as jnp
from jax import lax
from jax.experimental import pallas as pl
from jax.experimental.pallas import tpu as pltpu
from jax.sharding import PartitionSpec as P


ROWS = 1024
LOW = ROWS // 2
SUB = 8
STEP = 32
LANES = 128
MOST_PEERS = 16
VM = pl.BlockSpec(memory_space=pltpu.VMEM)
SM = pl.BlockSpec(memory_space=pltpu.SMEM)
HB = pl.BlockSpec(memory_space=pltpu.HBM)


def cost(flops, nbytes):
    return pl.CostEstimate(flops=int(flops), bytes_accessed=int(nbytes), transcendentals=0)


def room(mib):
    return pltpu.CompilerParams(vmem_limit_bytes=mib << 20)


def spread(values, group):
    take = lax.broadcasted_iota(jnp.int32, (SUB * STEP, SUB * STEP), 1)
    place = lax.broadcasted_iota(jnp.int32, (SUB * STEP, SUB * STEP), 0)
    swap = (take == (place % STEP) * SUB + ((place // STEP) ^ group)).astype(jnp.float32).astype(jnp.bfloat16)
    return [
        jnp.dot(swap, rows.reshape(SUB * STEP, rows.shape[-1]), preferred_element_type=jnp.float32).astype(jnp.bfloat16)
        for rows in values
    ]


def prep_body(grads, lookups, hot, notes, *refs):
    outs, (held, listed, sems, note_sems) = refs[:-4], refs[-4:]
    spd = grads.shape[0]
    me = lax.axis_index("tab")
    chunks = sems.shape[0]
    size = spd // chunks
    length = lookups.shape[1]
    moves = []
    for chunk in range(chunks):
        where = pl.ds(chunk * size, size)
        moves.append(pltpu.make_async_copy(grads.at[where], held.at[where], sems.at[chunk]))
        moves[-1].start()
    hot_move = pltpu.make_async_copy(hot, listed, note_sems.at[0])
    hot_move.start()
    note_move = pltpu.make_async_copy(lookups, notes.at[:, pl.ds(0, length)], note_sems.at[1])
    note_move.start()
    notes[:, pl.ds(length, LANES)] = jnp.full((1, LANES), -1, jnp.int32)
    relay = outs[-1]
    for chunk in range(chunks):
        lows = range(chunk * size, (chunk + 1) * size, STEP)
        moves[chunk].wait()
        for group in range(2):
            which = (me // SUB) ^ (1 - group)
            for low, turned in zip(lows, spread([held[pl.ds(low, STEP), which] for low in lows], me % SUB)):
                for at in range(SUB):
                    rows = turned[at * STEP:(at + 1) * STEP]
                    if group == 0:
                        outs[at][pl.ds(low, STEP), :] = rows
                    elif at < SUB // 2:
                        outs[at][pl.ds(spd + low, STEP), :] = rows
                    else:
                        relay[pl.ds((at - SUB // 2) * spd + low, STEP), :] = rows
    hot_move.wait()
    notes[:, pl.ds(length, hot.shape[1])] = listed[...]
    note_move.wait()


def prep(grads, lookups, hot):
    spd, _, _, width = grads.shape

    def block(parts):
        return jax.ShapeDtypeStruct((parts * spd, width), jnp.bfloat16)

    half = SUB // 2
    kept = [pltpu.with_memory_space_constraint(x, pltpu.HBM) for x in (grads, lookups, hot)]
    return pl.pallas_call(
        prep_body,
        out_shape=(jax.ShapeDtypeStruct((1, lookups.shape[1] + LANES), jnp.int32),)
        + (block(2),) * half
        + (block(1),) * half
        + (block(half),),
        in_specs=[HB] * 3,
        out_specs=(VM,) * (SUB + 2),
        scratch_shapes=[
            pltpu.VMEM((spd, 2, SUB, width), jnp.bfloat16),
            pltpu.VMEM((1, hot.shape[1]), jnp.int32),
            pltpu.SemaphoreType.DMA((4,)),
            pltpu.SemaphoreType.DMA((2,)),
        ],
        compiler_params=room(5),
        cost_estimate=cost(2 * SUB * spd * width * 512, 2 * SUB * spd * width * 4),
        name="prep",
    )(*kept)


def match_body(notes, low_match, high_side, hot_match):
    total = low_match.shape[1]
    size = LANES
    half = lax.axis_index("tab") // (lax.axis_size("tab") // 2)
    quarter = LOW // 2
    lows = lax.broadcasted_iota(jnp.int32, (quarter, size), 0).astype(jnp.float32).astype(jnp.bfloat16)
    one, zero = jnp.bfloat16(1), jnp.bfloat16(0)
    hot = notes[:, pl.ds(notes.shape[1] - LANES, LANES)].astype(jnp.float32)
    hot = jnp.broadcast_to(hot, (LANES, LANES)).T[:hot_match.shape[0]]
    for start in range(0, total, size):
        ids = notes[:, pl.ds(pl.multiple_of(half * total + start, size), size)]
        same = jnp.where(hot == ids.astype(jnp.float32), 1.0, 0.0)
        hot_match[:, pl.ds(start, size)] = same.astype(jnp.bfloat16)
        cold = (1.0 - jnp.sum(same, axis=0, keepdims=True)).astype(jnp.bfloat16)
        low = (ids % quarter).astype(jnp.float32).astype(jnp.bfloat16)
        middle = ((ids // quarter) % 2).astype(jnp.float32).astype(jnp.bfloat16)
        match = jnp.where(low == lows, one, zero)
        for top in range(2):
            keep = jnp.where(middle == jnp.bfloat16(top), cold, jnp.zeros_like(cold))
            low_match[pl.ds(top * quarter, quarter), pl.ds(start, size)] = match * keep
        high = (ids // LOW).astype(jnp.float32)
        high_side[pl.ds(start, size), :] = jnp.broadcast_to(high, (LANES, size)).T.astype(jnp.bfloat16)


def match(notes, total, hots):
    return pl.pallas_call(
        match_body,
        out_shape=(
            jax.ShapeDtypeStruct((LOW, total), jnp.bfloat16),
            jax.ShapeDtypeStruct((total, LANES), jnp.bfloat16),
            jax.ShapeDtypeStruct((hots, total), jnp.bfloat16),
        ),
        in_specs=[VM],
        out_specs=(VM,) * 3,
        compiler_params=room(8),
        cost_estimate=cost(LOW * total * 400, LOW * total * 2),
    )(notes)


def gather(spd, pieces, high_side, both, rows):
    width = rows.shape[1]
    near = lax.axis_size("tab") // 2
    me = lax.axis_index("tab") % near
    for shift, chunk, first in pieces:
        where = pl.ds(pl.multiple_of((me ^ shift) * spd, spd), spd)
        piece = chunk[pl.ds(first, spd), :]
        upper = piece * high_side[where, :]
        both[where, :width] = piece - upper
        both[where, width:] = upper
        rows[where, :] = piece


def split(value):
    half = value.shape[0] // 2
    lower, upper = value[:half], value[half:]
    first = lax.axis_index("rep") == 0
    return jnp.where(first, lower, upper), jnp.where(first, upper, lower)


def other_body(low_match, high_side, hot_match, *refs):
    chunks, (out, given, both, rows) = refs[:-4], refs[-4:]
    spd = rows.shape[0] // len(chunks)
    gather(spd, [(at, chunk, 0) for at, chunk in enumerate(chunks)], high_side, both, rows)
    width = rows.shape[1]
    hot = jnp.dot(hot_match[...], rows[...], preferred_element_type=jnp.float32)
    kept, given[...] = split(hot)
    part = jnp.dot(low_match[...], both[...], preferred_element_type=jnp.float32)
    for top in range(2):
        out[pl.ds(top * LOW, LOW), :] = part[:, top * width:(top + 1) * width].astype(jnp.bfloat16)
    out[pl.ds(ROWS, kept.shape[0]), :] = kept.astype(jnp.bfloat16)


def scratch(matched, width):
    total = matched[1].shape[0]
    return [pltpu.VMEM((total, 2 * width), jnp.bfloat16), pltpu.VMEM((total, width), jnp.bfloat16)]


def other_sums(chunks, matched):
    width = chunks[0].shape[1]
    total, half = matched[1].shape[0], matched[2].shape[0] // 2
    return pl.pallas_call(
        other_body,
        out_shape=(
            jax.ShapeDtypeStruct((ROWS + half, width), jnp.bfloat16),
            jax.ShapeDtypeStruct((half, width), jnp.float32),
        ),
        in_specs=[VM] * (3 + len(chunks)),
        out_specs=(VM, VM),
        scratch_shapes=scratch(matched, width),
        compiler_params=room(8),
        cost_estimate=cost(2 * total * width * ROWS, total * width * 2),
        name="other_sums",
    )(*matched, *chunks)


def project(values, matrix):
    high = values.astype(jnp.bfloat16)
    low = (values - high.astype(jnp.float32)).astype(jnp.bfloat16)
    return jnp.dot(high, matrix, preferred_element_type=jnp.float32) + jnp.dot(
        low, matrix, preferred_element_type=jnp.float32
    )


def partial_sums(spd, pieces, low_match, high_side, hot_match):
    near = lax.axis_size("tab") // 2
    me = lax.axis_index("tab") % near
    sides, lows, hots, rows = [], [], [], []
    for shift, chunk, first in pieces:
        where = pl.ds(pl.multiple_of((me ^ shift) * spd, spd), spd)
        piece = chunk[pl.ds(first, spd), :]
        upper = piece * high_side[where, :]
        sides.append(jnp.concatenate([piece - upper, upper], axis=1))
        lows.append(low_match[:, where])
        hots.append(hot_match[:, where])
        rows.append(piece)
    both = jnp.dot(jnp.concatenate(lows, axis=1), jnp.concatenate(sides, axis=0), preferred_element_type=jnp.float32)
    hot = jnp.dot(jnp.concatenate(hots, axis=1), jnp.concatenate(rows, axis=0), preferred_element_type=jnp.float32)
    return both, hot


def early_body(low_match, high_side, hot_match, own, one, two, three, relayed, total, hot):
    spd = own.shape[0] // 2
    pieces = [(0, own, spd), (1, one, spd), (2, two, spd), (3, three, spd), (4, relayed, 0)]
    total[...], hot[...] = partial_sums(spd, pieces, low_match, high_side, hot_match)


def early_sums(matched, chunks):
    width = chunks[0].shape[1]
    count = matched[1].shape[0]
    return pl.pallas_call(
        early_body,
        out_shape=(
            jax.ShapeDtypeStruct((LOW, 2 * width), jnp.float32),
            jax.ShapeDtypeStruct((matched[2].shape[0], width), jnp.float32),
        ),
        in_specs=[VM] * 8,
        out_specs=(VM, VM),
        compiler_params=room(8),
        cost_estimate=cost(count * width * ROWS, count * width * 2),
        name="early_sums",
    )(*matched, *chunks)


def own_body(widths, proj, low_match, high_side, hot_match, total, hot, *refs):
    chunks, (done, matrix, kept, given) = refs[:-4], refs[-4:]
    spd, width = chunks[0].shape
    columns = lax.broadcasted_iota(jnp.int32, proj.shape, 1)
    limit = widths[lax.axis_index("tab")]
    matrix[...] = jnp.where(columns < limit, proj[...].astype(jnp.float32), 0.0).astype(jnp.bfloat16)
    pieces = [(5 + at, chunk, 0) for at, chunk in enumerate(chunks)]
    both, more = partial_sums(spd, pieces, low_match, high_side, hot_match)
    kept[...], given[...] = split(hot[...] + more)
    both += total[...]
    for top in range(2):
        done[pl.ds(top * LOW, LOW), :] = project(both[:, top * width:(top + 1) * width], matrix[...])


def own_sums(matched, early, chunks, proj, widths):
    width = chunks[0].shape[1]
    count, half = matched[1].shape[0], matched[2].shape[0] // 2
    part = jax.ShapeDtypeStruct((half, width), jnp.float32)
    return pl.pallas_call(
        own_body,
        out_shape=(
            jax.ShapeDtypeStruct((ROWS, width), jnp.float32),
            jax.ShapeDtypeStruct((width, width), jnp.bfloat16),
            part,
            part,
        ),
        in_specs=[SM] + [VM] * (6 + len(chunks)),
        out_specs=(VM,) * 4,
        compiler_params=room(8),
        cost_estimate=cost(count * width * ROWS, count * width * 2),
        name="own_sums",
    )(widths, proj, *matched, *early, *chunks)


def cut_body(block, *outs):
    spd = outs[0].shape[0]
    for at, out in enumerate(outs):
        out[...] = block[pl.ds((at + 1) * spd, spd), :]


def cut(block, parts):
    spd, width = block.shape[0] // parts, block.shape[1]
    return pl.pallas_call(
        cut_body,
        out_shape=(jax.ShapeDtypeStruct((spd, width), block.dtype),) * (parts - 1),
        in_specs=[VM],
        out_specs=(VM,) * (parts - 1),
        compiler_params=room(2),
        cost_estimate=cost(block.size * 20, block.size * 4),
        name="cut",
    )(block)


PIECES = 4


def last_body(done, matrix, kept, far, same_chip, far_chip, cold, hot, held, sems):
    size = ROWS // PIECES
    table = matrix[...]
    moves = []
    for piece in range(PIECES):
        where = pl.ds(piece * size, size)
        held[where, :] = done[where, :] + jnp.dot(far[where, :], table, preferred_element_type=jnp.float32)
        moves.append(pltpu.make_async_copy(held.at[where], cold.at[where], sems.at[piece]))
        moves[-1].start()
    hot_far = far[pl.ds(ROWS, hot.shape[0]), :].astype(jnp.float32)
    hot[...] = project(kept[...] + hot_far + same_chip[...] + far_chip[...], table)
    for one in moves:
        one.wait()


def last(done, matrix, kept, far, same_chip, far_chip):
    half, width = same_chip.shape
    return pl.pallas_call(
        last_body,
        out_shape=(
            jax.ShapeDtypeStruct((ROWS, width), jnp.float32),
            jax.ShapeDtypeStruct((half, width), jnp.float32),
        ),
        in_specs=[VM] * 6,
        out_specs=(HB, VM),
        scratch_shapes=[
            pltpu.VMEM((ROWS, width), jnp.float32),
            pltpu.SemaphoreType.DMA((PIECES,)),
        ],
        compiler_params=room(4),
        cost_estimate=cost(4 * ROWS * width * width, ROWS * width * 10),
        name="last",
    )(done, matrix, kept, far, same_chip, far_chip)


def swap_reps(block):
    reps = lax.axis_size("rep")
    return lax.ppermute(block, "rep", [(r, r ^ 1) for r in range(reps)])


FIRST = (7, 6, 5, 4, 3, 2, 1)
PLANE = (1, 2, 3)


def shards(grad_out, indices, projections, widths, hot_ids):
    count, reps = lax.axis_size("tab"), lax.axis_size("rep")
    spd, tables, width = grad_out.shape
    half_len = count // 2 * spd
    hots = hot_ids.shape[1]
    grads = grad_out.reshape(spd, tables // SUB, SUB, width)

    def send(block, shift):
        return lax.ppermute(block, "tab", [(i, i ^ shift) for i in range(count)])

    notes, *blocks, relay = prep(grads, indices, hot_ids)
    got = {0: blocks[0]}
    for shift in FIRST:
        got[shift] = send(blocks[shift], shift)
    far_notes = send(notes, SUB)
    relayed = send(relay, SUB // 2)
    far_matched = match(far_notes, half_len, hots)
    partial, far_given = other_sums([got[shift] for shift in range(SUB)], far_matched)
    far = send(partial, SUB)
    pieces = cut(relayed, SUB // 2)
    second = [send(pieces[shift - 1], shift) for shift in PLANE]
    far_chip = lax.ppermute(
        far_given,
        ("rep", "tab"),
        [(r * count + i, (r ^ 1) * count + (i ^ SUB)) for r in range(reps) for i in range(count)],
    )
    own_matched = match(notes, half_len, hots)
    early = early_sums(own_matched, [got[0], got[1], got[2], got[3], relayed])
    done, matrix, kept, given = own_sums(own_matched, early, second, projections[0], widths)
    same_chip = swap_reps(given)
    cold, hot = last(done, matrix, kept, far, same_chip, far_chip)
    return cold[None, None], hot[None]


def block_sums(narrow_rows, lookups):
    total_len = narrow_rows.shape[0]
    block_len = math.gcd(total_len, 4096)
    positions = lax.broadcasted_iota(jnp.int32, (1, ROWS), 1)

    def add_block(block, totals):
        piece_rows = lax.dynamic_slice_in_dim(narrow_rows, block * block_len, block_len, 0)
        row_ids = lax.dynamic_slice_in_dim(lookups, block * block_len, block_len, 0)
        onehot = (row_ids[:, None] == positions).astype(jnp.bfloat16)
        return totals + lax.dot_general(
            onehot, piece_rows, (((0,), (0,)), ((), ())), preferred_element_type=jnp.float32
        )

    start_sums = jnp.zeros((ROWS, narrow_rows.shape[1]), jnp.float32)
    return lax.fori_loop(0, total_len // block_len, add_block, start_sums)


def many_shards(grad_out, indices, projections, widths, hot_ids):
    columns = lax.broadcasted_iota(jnp.int32, (1, projections.shape[2]), 1)
    limit = lax.dynamic_slice_in_dim(widths, lax.axis_index("tab"), 1, 0)
    received = lax.all_to_all(grad_out, "tab", split_axis=1, concat_axis=0, tiled=True)
    full_proj = jnp.einsum("be,ej->bj", received[:, 0], projections[0], preferred_element_type=jnp.float32)
    narrow = jnp.where(columns < limit[:, None], full_proj, 0.0).astype(jnp.bfloat16)
    row_grads = block_sums(narrow, indices[0])
    own_hot = row_grads[hot_ids[0]]
    half_hot = own_hot.shape[0] // 2
    replica = lax.axis_index("rep")
    kept_rows = lax.dynamic_slice_in_dim(own_hot, replica * half_hot, half_hot, 0)
    given_rows = lax.dynamic_slice_in_dim(own_hot, (1 - replica) * half_hot, half_hot, 0)
    hot_grad = kept_rows + swap_reps(given_rows)
    all_rows = lax.broadcasted_iota(jnp.int32, (ROWS, 1), 0)
    is_hot = jnp.any(hot_ids == all_rows, axis=1)
    cold_grad = jnp.where(is_hot[:, None], jnp.float32(0.0), row_grads)
    return cold_grad[None, None], hot_grad[None]


def solution(mesh):
    placed = (
        P(("rep", "tab"), None, None),
        P("tab", "rep"),
        P("tab", None, None),
        P(),
        P("tab", None),
    )
    few = mesh.shape["tab"] <= MOST_PEERS
    return jax.shard_map(
        shards if few else many_shards,
        mesh=mesh,
        in_specs=placed,
        out_specs=(P("rep", "tab", None, None), P("tab", "rep", None)),
        check_vma=False,
    )
```

```python
import functools
import math

import jax
import jax.numpy as jnp
from jax import lax
from jax.experimental import pallas as pl
from jax.experimental.pallas import tpu as pltpu
from jax.sharding import PartitionSpec as P


ROWS = 1024
LOW = ROWS // 2
SUB = 8
STEP = 32
LANES = 128
MOST_PEERS = 16
VM = pl.BlockSpec(memory_space=pltpu.VMEM)
SM = pl.BlockSpec(memory_space=pltpu.SMEM)
HB = pl.BlockSpec(memory_space=pltpu.HBM)


def cost(flops, nbytes):
    return pl.CostEstimate(flops=int(flops), bytes_accessed=int(nbytes), transcendentals=0)


def room(mib):
    return pltpu.CompilerParams(vmem_limit_bytes=mib << 20)


def spread(values, group):
    take = lax.broadcasted_iota(jnp.int32, (SUB * STEP, SUB * STEP), 1)
    place = lax.broadcasted_iota(jnp.int32, (SUB * STEP, SUB * STEP), 0)
    swap = (take == (place % STEP) * SUB + ((place // STEP) ^ group)).astype(jnp.float32).astype(jnp.bfloat16)
    return [
        jnp.dot(swap, rows.reshape(SUB * STEP, rows.shape[-1]), preferred_element_type=jnp.float32).astype(jnp.bfloat16)
        for rows in values
    ]


def prep_body(grads, lookups, hot, notes, *refs):
    outs, (held, listed, sems, note_sems) = refs[:-4], refs[-4:]
    planes = outs[SUB:-1]
    spd = grads.shape[0]
    me = lax.axis_index("tab")
    chunks = sems.shape[0]
    size = spd // chunks
    length = lookups.shape[1]
    moves = []
    for chunk in range(chunks):
        where = pl.ds(chunk * size, size)
        moves.append(pltpu.make_async_copy(grads.at[where], held.at[where], sems.at[chunk]))
        moves[-1].start()
    hot_move = pltpu.make_async_copy(hot, listed, note_sems.at[0])
    hot_move.start()
    note_move = pltpu.make_async_copy(lookups, notes.at[:, pl.ds(0, length)], note_sems.at[1])
    note_move.start()
    notes[:, pl.ds(length, LANES)] = jnp.full((1, LANES), -1, jnp.int32)
    relay = outs[-1]
    for chunk in range(chunks):
        lows = range(chunk * size, (chunk + 1) * size, STEP)
        moves[chunk].wait()
        for group in range(2):
            which = (me // SUB) ^ (1 - group)
            for low, turned in zip(lows, spread([held[pl.ds(low, STEP), which] for low in lows], me % SUB)):
                for at in range(SUB):
                    rows = turned[at * STEP:(at + 1) * STEP]
                    if group == 0:
                        outs[at][pl.ds(low, STEP), :] = rows
                    elif at in SPLIT:
                        planes[SPLIT.index(at)][pl.ds(low, STEP), :] = rows
                    elif at < SUB // 2:
                        outs[at][pl.ds(spd + low, STEP), :] = rows
                    else:
                        relay[pl.ds((at - SUB // 2) * spd + low, STEP), :] = rows
    hot_move.wait()
    notes[:, pl.ds(length, hot.shape[1])] = listed[...]
    note_move.wait()


def prep(grads, lookups, hot):
    spd, _, _, width = grads.shape

    def block(parts):
        return jax.ShapeDtypeStruct((parts * spd, width), jnp.bfloat16)

    half = SUB // 2
    kept = [pltpu.with_memory_space_constraint(x, pltpu.HBM) for x in (grads, lookups, hot)]
    return pl.pallas_call(
        prep_body,
        out_shape=(jax.ShapeDtypeStruct((1, lookups.shape[1] + LANES), jnp.int32),)
        + tuple(block(1 if shift in SPLIT or shift >= half else 2) for shift in range(SUB))
        + (block(1),) * len(SPLIT)
        + (block(half),),
        in_specs=[HB] * 3,
        out_specs=(VM,) * (SUB + 2 + len(SPLIT)),
        scratch_shapes=[
            pltpu.VMEM((spd, 2, SUB, width), jnp.bfloat16),
            pltpu.VMEM((1, hot.shape[1]), jnp.int32),
            pltpu.SemaphoreType.DMA((4,)),
            pltpu.SemaphoreType.DMA((2,)),
        ],
        compiler_params=room(5),
        cost_estimate=cost(2 * SUB * spd * width * 512, 2 * SUB * spd * width * 4),
        name="prep",
    )(*kept)


def fill_match(notes, low_match, high_side, hot_match):
    total = low_match.shape[1]
    size = LANES
    half = lax.axis_index("tab") // (lax.axis_size("tab") // 2)
    quarter = LOW // 2
    lows = lax.broadcasted_iota(jnp.int32, (quarter, size), 0).astype(jnp.float32).astype(jnp.bfloat16)
    one, zero = jnp.bfloat16(1), jnp.bfloat16(0)
    hot = notes[:, pl.ds(notes.shape[1] - LANES, LANES)].astype(jnp.float32)
    hot = jnp.broadcast_to(hot, (LANES, LANES)).T[:hot_match.shape[0]]
    for start in range(0, total, size):
        ids = notes[:, pl.ds(pl.multiple_of(half * total + start, size), size)]
        same = jnp.where(hot == ids.astype(jnp.float32), 1.0, 0.0)
        hot_match[:, pl.ds(start, size)] = same.astype(jnp.bfloat16)
        cold = (1.0 - jnp.sum(same, axis=0, keepdims=True)).astype(jnp.bfloat16)
        low = (ids % quarter).astype(jnp.float32).astype(jnp.bfloat16)
        middle = ((ids // quarter) % 2).astype(jnp.float32).astype(jnp.bfloat16)
        match = jnp.where(low == lows, one, zero)
        for top in range(2):
            keep = jnp.where(middle == jnp.bfloat16(top), cold, jnp.zeros_like(cold))
            low_match[pl.ds(top * quarter, quarter), pl.ds(start, size)] = match * keep
        high = (ids // LOW).astype(jnp.float32)
        high_side[pl.ds(start, size), :] = jnp.broadcast_to(high, (LANES, size)).T.astype(jnp.bfloat16)


def match(notes, total, hots):
    return pl.pallas_call(
        fill_match,
        out_shape=(
            jax.ShapeDtypeStruct((LOW, total), jnp.bfloat16),
            jax.ShapeDtypeStruct((total, LANES), jnp.bfloat16),
            jax.ShapeDtypeStruct((hots, total), jnp.bfloat16),
        ),
        in_specs=[VM],
        out_specs=(VM,) * 3,
        compiler_params=room(8),
        cost_estimate=cost(LOW * total * 400, LOW * total * 2),
    )(notes)


def split(value):
    half = value.shape[0] // 2
    lower, upper = value[:half], value[half:]
    first = lax.axis_index("rep") == 0
    return jnp.where(first, lower, upper), jnp.where(first, upper, lower)


def project(values, matrix):
    high = values.astype(jnp.bfloat16)
    low = (values - high.astype(jnp.float32)).astype(jnp.bfloat16)
    return jnp.dot(high, matrix, preferred_element_type=jnp.float32) + jnp.dot(
        low, matrix, preferred_element_type=jnp.float32
    )


def partial_sums(spd, pieces, low_match, high_side, hot_match, matrix=None):
    near = lax.axis_size("tab") // 2
    me = lax.axis_index("tab") % near
    sides, lows, hots, rows = [], [], [], []
    for shift, first, chunk in pieces:
        where = pl.ds(pl.multiple_of((me ^ shift) * spd, spd), spd)
        piece = chunk[pl.ds(first, spd), :]
        if matrix is not None:
            piece = jnp.dot(piece, matrix, preferred_element_type=jnp.float32).astype(jnp.bfloat16)
        upper = piece * high_side[where, :]
        sides.append(jnp.concatenate([piece - upper, upper], axis=1))
        lows.append(low_match[:, where])
        hots.append(hot_match[:, where])
        rows.append(piece)
    both = jnp.dot(jnp.concatenate(lows, axis=1), jnp.concatenate(sides, axis=0), preferred_element_type=jnp.float32)
    hot = jnp.dot(jnp.concatenate(hots, axis=1), jnp.concatenate(rows, axis=0), preferred_element_type=jnp.float32)
    return both, hot


def early_body(spd, places, low_match, high_side, hot_match, *refs):
    chunks, (total, hot) = refs[:-2], refs[-2:]
    pieces = [place + (chunk,) for place, chunk in zip(places, chunks)]
    total[...], hot[...] = partial_sums(spd, pieces, low_match, high_side, hot_match)


def own_early_body(spd, places, widths, proj, low_match, high_side, hot_match, *refs):
    chunks, (total, hot, matrix) = refs[:-3], refs[-3:]
    columns = lax.broadcasted_iota(jnp.int32, proj.shape, 1)
    limit = widths[lax.axis_index("tab")]
    matrix[...] = jnp.where(columns < limit, proj[...].astype(jnp.float32), 0.0).astype(jnp.bfloat16)
    pieces = [place + (chunk,) for place, chunk in zip(places, chunks)]
    total[...], hot[...] = partial_sums(spd, pieces, low_match, high_side, hot_match, matrix[...])


def early_sums(spd, matched, items, widths=None, proj=None):
    places, chunks = tuple(item[:2] for item in items), [item[2] for item in items]
    width = chunks[0].shape[1]
    shapes = (
        jax.ShapeDtypeStruct((LOW, 2 * width), jnp.float32),
        jax.ShapeDtypeStruct((matched[2].shape[0], width), jnp.float32),
    )
    own = proj is not None
    if own:
        shapes += (jax.ShapeDtypeStruct(proj.shape, jnp.bfloat16),)
    return pl.pallas_call(
        functools.partial(own_early_body if own else early_body, spd, places),
        out_shape=shapes,
        in_specs=([SM, VM] if own else []) + [VM] * (3 + len(chunks)),
        out_specs=(VM,) * len(shapes),
        compiler_params=room(8),
        cost_estimate=cost(2 * spd * len(chunks) * width * ROWS, spd * len(chunks) * width * 2),
        name="own_early" if own else "far_early",
    )(*([widths, proj] if own else []), *matched, *chunks)


def other_body(spd, places, low_match, high_side, hot_match, total, hot, *refs):
    chunks, (lower, upper, given) = refs[:-3], refs[-3:]
    pieces = [place + (chunk,) for place, chunk in zip(places, chunks)]
    both, more = partial_sums(spd, pieces, low_match, high_side, hot_match)
    both += total[...]
    width = lower.shape[1]
    kept, given[...] = split(hot[...] + more)
    lower[...] = both[:, :width].astype(jnp.bfloat16)
    upper[pl.ds(0, LOW), :] = both[:, width:].astype(jnp.bfloat16)
    upper[pl.ds(LOW, kept.shape[0]), :] = kept.astype(jnp.bfloat16)


def other_sums(spd, matched, early, items):
    places, chunks = tuple(item[:2] for item in items), [item[2] for item in items]
    width, half = chunks[0].shape[1], matched[2].shape[0] // 2
    return pl.pallas_call(
        functools.partial(other_body, spd, places),
        out_shape=(
            jax.ShapeDtypeStruct((LOW, width), jnp.bfloat16),
            jax.ShapeDtypeStruct((LOW + half, width), jnp.bfloat16),
            jax.ShapeDtypeStruct((half, width), jnp.float32),
        ),
        in_specs=[VM] * (5 + len(chunks)),
        out_specs=(VM,) * 3,
        compiler_params=room(8),
        cost_estimate=cost(2 * spd * len(chunks) * width * ROWS, spd * len(chunks) * width * 2),
        name="other_sums",
    )(*matched, *early, *chunks)


def own_body(spd, places, matrix, low_match, high_side, hot_match, total, hot, *refs):
    chunks, (done, kept, given) = refs[:-3], refs[-3:]
    pieces = [place + (chunk,) for place, chunk in zip(places, chunks)]
    both, more = partial_sums(spd, pieces, low_match, high_side, hot_match, matrix[...])
    kept[...], given[...] = split(hot[...] + more)
    width = done.shape[1]
    for top in range(2):
        where = slice(top * width, (top + 1) * width)
        done[pl.ds(top * LOW, LOW), :] = both[:, where] + total[:, where]


def own_sums(spd, matched, early, items, matrix):
    places, chunks = tuple(item[:2] for item in items), [item[2] for item in items]
    width, half = chunks[0].shape[1], matched[2].shape[0] // 2
    part = jax.ShapeDtypeStruct((half, width), jnp.float32)
    return pl.pallas_call(
        functools.partial(own_body, spd, places),
        out_shape=(jax.ShapeDtypeStruct((ROWS, width), jnp.float32), part, part),
        in_specs=[VM] * (6 + len(chunks)),
        out_specs=(VM,) * 3,
        compiler_params=room(8),
        cost_estimate=cost(2 * spd * len(chunks) * width * ROWS, spd * len(chunks) * width * 2),
        name="own_sums",
    )(matrix, *matched, *early, *chunks)


def cut_body(block, *outs):
    spd = outs[0].shape[0]
    for at, out in enumerate(outs):
        out[...] = block[pl.ds((at + 1) * spd, spd), :]


def cut(block, parts):
    spd, width = block.shape[0] // parts, block.shape[1]
    return pl.pallas_call(
        cut_body,
        out_shape=(jax.ShapeDtypeStruct((spd, width), block.dtype),) * (parts - 1),
        in_specs=[VM],
        out_specs=(VM,) * (parts - 1),
        compiler_params=room(2),
        cost_estimate=cost(block.size * 20, block.size * 4),
        name="cut",
    )(block)


PIECES = 2


def write_rows(top, done, table, far, cold, held, sems):
    size = LOW // PIECES
    moves = []
    for piece in range(PIECES):
        where = pl.ds(top * LOW + piece * size, size)
        from_far = pl.ds(piece * size, size)
        held[from_far, :] = done[where, :] + jnp.dot(far[from_far, :], table, preferred_element_type=jnp.float32)
        moves.append(pltpu.make_async_copy(held.at[from_far], cold.at[where], sems.at[piece]))
        moves[-1].start()
    return moves


def lower_body(done, matrix, far, cold, held, sems):
    for one in write_rows(0, done, matrix[...], far, cold, held, sems):
        one.wait()


def last_scratch(width):
    return [pltpu.VMEM((LOW, width), jnp.float32), pltpu.SemaphoreType.DMA((PIECES,))]


def lower_part(done, matrix, far):
    width = far.shape[1]
    return pl.pallas_call(
        lower_body,
        out_shape=jax.ShapeDtypeStruct((ROWS, width), jnp.float32),
        in_specs=[VM] * 3,
        out_specs=HB,
        scratch_shapes=last_scratch(width),
        compiler_params=room(4),
        cost_estimate=cost(2 * ROWS * width * width, ROWS * width * 5),
        name="lower_part",
    )(done, matrix, far)


def upper_body(begun, done, matrix, kept, far, same_chip, far_chip, cold, hot, held, sems, hot_held, hot_sem):
    table = matrix[...]
    hot_far = far[pl.ds(LOW, hot.shape[0]), :].astype(jnp.float32)
    hot_held[...] = kept[...] + same_chip[...] + project(hot_far + far_chip[...], table)
    moves = [pltpu.make_async_copy(hot_held, hot, hot_sem)]
    moves[0].start()
    moves += write_rows(1, done, table, far, cold, held, sems)
    for one in moves:
        one.wait()


def upper_part(begun, done, matrix, kept, far, same_chip, far_chip):
    half, width = same_chip.shape
    return pl.pallas_call(
        upper_body,
        out_shape=(
            jax.ShapeDtypeStruct((ROWS, width), jnp.float32),
            jax.ShapeDtypeStruct((half, width), jnp.float32),
        ),
        in_specs=[HB] + [VM] * 6,
        out_specs=(HB, HB),
        scratch_shapes=last_scratch(width) + [pltpu.VMEM((half, width), jnp.float32), pltpu.SemaphoreType.DMA],
        input_output_aliases={0: 0},
        compiler_params=room(4),
        cost_estimate=cost(2 * ROWS * width * width, ROWS * width * 5),
        name="upper_part",
    )(begun, done, matrix, kept, far, same_chip, far_chip)


def swap_reps(block):
    reps = lax.axis_size("rep")
    return lax.ppermute(block, "rep", [(r, r ^ 1) for r in range(reps)])


FIRST = (7, 6, 5, 4, 3, 2, 1)
PLANE = (1, 2, 3)
SPLIT = ()
EARLY = (0, 4, 3, 7, 6, 5)


def shards(grad_out, indices, projections, widths, hot_ids):
    count, reps = lax.axis_size("tab"), lax.axis_size("rep")
    spd, tables, width = grad_out.shape
    half_len = count // 2 * spd
    hots = hot_ids.shape[1]
    grads = grad_out.reshape(spd, tables // SUB, SUB, width)

    def send(block, shift):
        return lax.ppermute(block, "tab", [(i, i ^ shift) for i in range(count)])

    notes, *blocks, relay = prep(grads, indices, hot_ids)
    got = {0: blocks[0]}
    for shift in FIRST:
        got[shift] = send(blocks[shift], shift)
    far_notes = send(notes, SUB)
    relayed = send(relay, SUB // 2)
    far_matched = match(far_notes, half_len, hots)
    far_early = early_sums(spd, far_matched, [(shift, 0, got[shift]) for shift in EARLY])
    lower, upper, far_given = other_sums(
        spd, far_matched, far_early, [(shift, 0, got[shift]) for shift in range(SUB) if shift not in EARLY]
    )
    far_lower = send(lower, SUB)
    far_upper = send(upper, SUB)
    own = [(shift, spd, got[shift]) for shift in (0,) + PLANE if shift not in SPLIT]
    own += [(shift, 0, send(block, shift)) for shift, block in zip(SPLIT, blocks[SUB:])]
    own += [(SUB // 2, 0, relayed)]
    pieces = cut(relayed, SUB // 2)
    second = [send(pieces[shift - 1], shift) for shift in PLANE]
    far_chip = lax.ppermute(
        far_given,
        ("rep", "tab"),
        [(r * count + i, (r ^ 1) * count + (i ^ SUB)) for r in range(reps) for i in range(count)],
    )
    own_matched = match(notes, half_len, hots)
    *own_early, matrix = early_sums(spd, own_matched, own, widths, projections[0])
    done, kept, given = own_sums(
        spd, own_matched, own_early, [(SUB // 2 + shift, 0, one) for shift, one in zip(PLANE, second)], matrix
    )
    same_chip = swap_reps(given)
    begun = lower_part(done, matrix, far_lower)
    cold, hot = upper_part(begun, done, matrix, kept, far_upper, same_chip, far_chip)
    return cold[None, None], hot[None]


def block_sums(narrow_rows, lookups):
    total_len = narrow_rows.shape[0]
    block_len = math.gcd(total_len, 4096)
    positions = lax.broadcasted_iota(jnp.int32, (1, ROWS), 1)

    def add_block(block, totals):
        piece_rows = lax.dynamic_slice_in_dim(narrow_rows, block * block_len, block_len, 0)
        row_ids = lax.dynamic_slice_in_dim(lookups, block * block_len, block_len, 0)
        onehot = (row_ids[:, None] == positions).astype(jnp.bfloat16)
        return totals + lax.dot_general(
            onehot, piece_rows, (((0,), (0,)), ((), ())), preferred_element_type=jnp.float32
        )

    start_sums = jnp.zeros((ROWS, narrow_rows.shape[1]), jnp.float32)
    return lax.fori_loop(0, total_len // block_len, add_block, start_sums)


def many_shards(grad_out, indices, projections, widths, hot_ids):
    columns = lax.broadcasted_iota(jnp.int32, (1, projections.shape[2]), 1)
    limit = lax.dynamic_slice_in_dim(widths, lax.axis_index("tab"), 1, 0)
    received = lax.all_to_all(grad_out, "tab", split_axis=1, concat_axis=0, tiled=True)
    full_proj = jnp.einsum("be,ej->bj", received[:, 0], projections[0], preferred_element_type=jnp.float32)
    narrow = jnp.where(columns < limit[:, None], full_proj, 0.0).astype(jnp.bfloat16)
    row_grads = block_sums(narrow, indices[0])
    own_hot = row_grads[hot_ids[0]]
    half_hot = own_hot.shape[0] // 2
    replica = lax.axis_index("rep")
    kept_rows = lax.dynamic_slice_in_dim(own_hot, replica * half_hot, half_hot, 0)
    given_rows = lax.dynamic_slice_in_dim(own_hot, (1 - replica) * half_hot, half_hot, 0)
    hot_grad = kept_rows + swap_reps(given_rows)
    all_rows = lax.broadcasted_iota(jnp.int32, (ROWS, 1), 0)
    is_hot = jnp.any(hot_ids == all_rows, axis=1)
    cold_grad = jnp.where(is_hot[:, None], jnp.float32(0.0), row_grads)
    return cold_grad[None, None], hot_grad[None]


def solution(mesh):
    placed = (
        P(("rep", "tab"), None, None),
        P("tab", "rep"),
        P("tab", None, None),
        P(),
        P("tab", None),
    )
    few = mesh.shape["tab"] <= MOST_PEERS
    return jax.shard_map(
        shards if few else many_shards,
        mesh=mesh,
        in_specs=placed,
        out_specs=(P("rep", "tab", None, None), P("tab", "rep", None)),
        check_vma=False,
    )
```

```python
import functools
import math

import jax
import jax.numpy as jnp
from jax import lax
from jax.experimental import pallas as pl
from jax.experimental.pallas import tpu as pltpu
from jax.sharding import PartitionSpec as P


ROWS = 1024
LOW = ROWS // 2
SUB = 8
STEP = 16
LANES = 128
MOST_PEERS = 16
VM = pl.BlockSpec(memory_space=pltpu.VMEM)
SM = pl.BlockSpec(memory_space=pltpu.SMEM)
HB = pl.BlockSpec(memory_space=pltpu.HBM)


def cost(flops, nbytes):
    return pl.CostEstimate(flops=int(flops), bytes_accessed=int(nbytes), transcendentals=0)


def room(mib):
    return pltpu.CompilerParams(vmem_limit_bytes=mib << 20)


def spread(values, group):
    take = lax.broadcasted_iota(jnp.int32, (SUB * STEP, SUB * STEP), 1)
    place = lax.broadcasted_iota(jnp.int32, (SUB * STEP, SUB * STEP), 0)
    swap = (take == (place % STEP) * SUB + ((place // STEP) ^ group)).astype(jnp.float32).astype(jnp.bfloat16)
    return [
        jnp.dot(swap, rows.reshape(SUB * STEP, rows.shape[-1]), preferred_element_type=jnp.float32).astype(jnp.bfloat16)
        for rows in values
    ]


def prep_body(grads, lookups, hot, notes, *refs):
    outs, (held, listed, sems, note_sems) = refs[:-4], refs[-4:]
    planes = outs[SUB:-1]
    spd = grads.shape[0]
    me = lax.axis_index("tab")
    chunks = sems.shape[0]
    size = spd // chunks
    length = lookups.shape[1]
    moves = []
    for chunk in range(chunks):
        where = pl.ds(chunk * size, size)
        moves.append(pltpu.make_async_copy(grads.at[where], held.at[where], sems.at[chunk]))
        moves[-1].start()
    hot_move = pltpu.make_async_copy(hot, listed, note_sems.at[0])
    hot_move.start()
    note_move = pltpu.make_async_copy(lookups, notes.at[:, pl.ds(0, length)], note_sems.at[1])
    note_move.start()
    notes[:, pl.ds(length, LANES)] = jnp.full((1, LANES), -1, jnp.int32)
    relay = outs[-1]
    for chunk in range(chunks):
        lows = range(chunk * size, (chunk + 1) * size, STEP)
        moves[chunk].wait()
        for group in range(2):
            which = (me // SUB) ^ (1 - group)
            for low, turned in zip(lows, spread([held[pl.ds(low, STEP), which] for low in lows], me % SUB)):
                for at in range(SUB):
                    rows = turned[at * STEP:(at + 1) * STEP]
                    if group == 0:
                        outs[at][pl.ds(low, STEP), :] = rows
                    elif at in SPLIT:
                        planes[SPLIT.index(at)][pl.ds(low, STEP), :] = rows
                    elif at < SUB // 2:
                        outs[at][pl.ds(spd + low, STEP), :] = rows
                    else:
                        relay[pl.ds((at - SUB // 2) * spd + low, STEP), :] = rows
    hot_move.wait()
    notes[:, pl.ds(length, hot.shape[1])] = listed[...]
    note_move.wait()


def prep(grads, lookups, hot):
    spd, _, _, width = grads.shape

    def block(parts):
        return jax.ShapeDtypeStruct((parts * spd, width), jnp.bfloat16)

    half = SUB // 2
    kept = [pltpu.with_memory_space_constraint(x, pltpu.HBM) for x in (grads, lookups, hot)]
    return pl.pallas_call(
        prep_body,
        out_shape=(jax.ShapeDtypeStruct((1, lookups.shape[1] + LANES), jnp.int32),)
        + tuple(block(1 if shift in SPLIT or shift >= half else 2) for shift in range(SUB))
        + (block(1),) * len(SPLIT)
        + (block(half),),
        in_specs=[HB] * 3,
        out_specs=(VM,) * (SUB + 2 + len(SPLIT)),
        scratch_shapes=[
            pltpu.VMEM((spd, 2, SUB, width), jnp.bfloat16),
            pltpu.VMEM((1, hot.shape[1]), jnp.int32),
            pltpu.SemaphoreType.DMA((2,)),
            pltpu.SemaphoreType.DMA((2,)),
        ],
        compiler_params=room(5),
        cost_estimate=cost(2 * SUB * spd * width * 512, 2 * SUB * spd * width * 4),
        name="prep",
    )(*kept)


def fill_match(notes, low_match, high_side, hot_match):
    total = low_match.shape[1]
    size = LANES
    half = lax.axis_index("tab") // (lax.axis_size("tab") // 2)
    quarter = LOW // 2
    lows = lax.broadcasted_iota(jnp.int32, (quarter, size), 0).astype(jnp.float32).astype(jnp.bfloat16)
    one, zero = jnp.bfloat16(1), jnp.bfloat16(0)
    hot = notes[:, pl.ds(notes.shape[1] - LANES, LANES)].astype(jnp.float32)
    hot = jnp.broadcast_to(hot, (LANES, LANES)).T[:hot_match.shape[0]]
    for start in range(0, total, size):
        ids = notes[:, pl.ds(pl.multiple_of(half * total + start, size), size)]
        same = jnp.where(hot == ids.astype(jnp.float32), 1.0, 0.0)
        hot_match[:, pl.ds(start, size)] = same.astype(jnp.bfloat16)
        cold = (1.0 - jnp.sum(same, axis=0, keepdims=True)).astype(jnp.bfloat16)
        low = (ids % quarter).astype(jnp.float32).astype(jnp.bfloat16)
        middle = ((ids // quarter) % 2).astype(jnp.float32).astype(jnp.bfloat16)
        match = jnp.where(low == lows, one, zero)
        for top in range(2):
            keep = jnp.where(middle == jnp.bfloat16(top), cold, jnp.zeros_like(cold))
            low_match[pl.ds(top * quarter, quarter), pl.ds(start, size)] = match * keep
        high = (ids // LOW).astype(jnp.float32)
        high_side[pl.ds(start, size), :] = jnp.broadcast_to(high, (LANES, size)).T.astype(jnp.bfloat16)


def match(notes, total, hots):
    return pl.pallas_call(
        fill_match,
        out_shape=(
            jax.ShapeDtypeStruct((LOW, total), jnp.bfloat16),
            jax.ShapeDtypeStruct((total, LANES), jnp.bfloat16),
            jax.ShapeDtypeStruct((hots, total), jnp.bfloat16),
        ),
        in_specs=[VM],
        out_specs=(VM,) * 3,
        compiler_params=room(8),
        cost_estimate=cost(LOW * total * 400, LOW * total * 2),
    )(notes)


def split(value):
    half = value.shape[0] // 2
    lower, upper = value[:half], value[half:]
    first = lax.axis_index("rep") == 0
    return jnp.where(first, lower, upper), jnp.where(first, upper, lower)


def project(values, matrix):
    high = values.astype(jnp.bfloat16)
    low = (values - high.astype(jnp.float32)).astype(jnp.bfloat16)
    return jnp.dot(high, matrix, preferred_element_type=jnp.float32) + jnp.dot(
        low, matrix, preferred_element_type=jnp.float32
    )


def partial_sums(spd, pieces, low_match, high_side, hot_match, matrix=None):
    near = lax.axis_size("tab") // 2
    me = lax.axis_index("tab") % near
    sides, lows, hots, rows = [], [], [], []
    for shift, first, chunk in pieces:
        where = pl.ds(pl.multiple_of((me ^ shift) * spd, spd), spd)
        piece = chunk[pl.ds(first, spd), :]
        if matrix is not None:
            piece = jnp.dot(piece, matrix, preferred_element_type=jnp.float32).astype(jnp.bfloat16)
        upper = piece * high_side[where, :]
        sides.append(jnp.concatenate([piece - upper, upper], axis=1))
        lows.append(low_match[:, where])
        hots.append(hot_match[:, where])
        rows.append(piece)
    both = jnp.dot(jnp.concatenate(lows, axis=1), jnp.concatenate(sides, axis=0), preferred_element_type=jnp.float32)
    hot = jnp.dot(jnp.concatenate(hots, axis=1), jnp.concatenate(rows, axis=0), preferred_element_type=jnp.float32)
    return both, hot


def early_body(spd, places, low_match, high_side, hot_match, *refs):
    chunks, (total, hot) = refs[:-2], refs[-2:]
    pieces = [place + (chunk,) for place, chunk in zip(places, chunks)]
    total[...], hot[...] = partial_sums(spd, pieces, low_match, high_side, hot_match)


def own_early_body(spd, places, widths, proj, low_match, high_side, hot_match, *refs):
    chunks, (total, hot, matrix) = refs[:-3], refs[-3:]
    columns = lax.broadcasted_iota(jnp.int32, proj.shape, 1)
    limit = widths[lax.axis_index("tab")]
    matrix[...] = jnp.where(columns < limit, proj[...].astype(jnp.float32), 0.0).astype(jnp.bfloat16)
    pieces = [place + (chunk,) for place, chunk in zip(places, chunks)]
    total[...], hot[...] = partial_sums(spd, pieces, low_match, high_side, hot_match, matrix[...])


def early_sums(spd, matched, items, widths=None, proj=None):
    places, chunks = tuple(item[:2] for item in items), [item[2] for item in items]
    width = chunks[0].shape[1]
    shapes = (
        jax.ShapeDtypeStruct((LOW, 2 * width), jnp.float32),
        jax.ShapeDtypeStruct((matched[2].shape[0], width), jnp.float32),
    )
    own = proj is not None
    if own:
        shapes += (jax.ShapeDtypeStruct(proj.shape, jnp.bfloat16),)
    return pl.pallas_call(
        functools.partial(own_early_body if own else early_body, spd, places),
        out_shape=shapes,
        in_specs=([SM, VM] if own else []) + [VM] * (3 + len(chunks)),
        out_specs=(VM,) * len(shapes),
        compiler_params=room(8),
        cost_estimate=cost(2 * spd * len(chunks) * width * ROWS, spd * len(chunks) * width * 2),
        name="own_early" if own else "far_early",
    )(*([widths, proj] if own else []), *matched, *chunks)


def other_body(spd, places, low_match, high_side, hot_match, total, hot, *refs):
    chunks, (out, given) = refs[:-2], refs[-2:]
    pieces = [place + (chunk,) for place, chunk in zip(places, chunks)]
    both, more = partial_sums(spd, pieces, low_match, high_side, hot_match)
    both += total[...]
    width = out.shape[1]
    kept, given[...] = split(hot[...] + more)
    for top in range(2):
        out[pl.ds(top * LOW, LOW), :] = both[:, top * width:(top + 1) * width].astype(jnp.bfloat16)
    out[pl.ds(ROWS, kept.shape[0]), :] = kept.astype(jnp.bfloat16)


def other_sums(spd, matched, early, items):
    places, chunks = tuple(item[:2] for item in items), [item[2] for item in items]
    width, half = chunks[0].shape[1], matched[2].shape[0] // 2
    return pl.pallas_call(
        functools.partial(other_body, spd, places),
        out_shape=(
            jax.ShapeDtypeStruct((ROWS + half, width), jnp.bfloat16),
            jax.ShapeDtypeStruct((half, width), jnp.float32),
        ),
        in_specs=[VM] * (5 + len(chunks)),
        out_specs=(VM,) * 2,
        compiler_params=room(8),
        cost_estimate=cost(2 * spd * len(chunks) * width * ROWS, spd * len(chunks) * width * 2),
        name="other_sums",
    )(*matched, *early, *chunks)


def own_body(spd, places, matrix, low_match, high_side, hot_match, total, hot, *refs):
    chunks, (done, kept, given) = refs[:-3], refs[-3:]
    pieces = [place + (chunk,) for place, chunk in zip(places, chunks)]
    both, more = partial_sums(spd, pieces, low_match, high_side, hot_match, matrix[...])
    kept[...], given[...] = split(hot[...] + more)
    width = done.shape[1]
    for top in range(2):
        where = slice(top * width, (top + 1) * width)
        done[pl.ds(top * LOW, LOW), :] = both[:, where] + total[:, where]


def own_sums(spd, matched, early, items, matrix):
    places, chunks = tuple(item[:2] for item in items), [item[2] for item in items]
    width, half = chunks[0].shape[1], matched[2].shape[0] // 2
    part = jax.ShapeDtypeStruct((half, width), jnp.float32)
    return pl.pallas_call(
        functools.partial(own_body, spd, places),
        out_shape=(jax.ShapeDtypeStruct((ROWS, width), jnp.float32), part, part),
        in_specs=[VM] * (6 + len(chunks)),
        out_specs=(VM,) * 3,
        compiler_params=room(8),
        cost_estimate=cost(2 * spd * len(chunks) * width * ROWS, spd * len(chunks) * width * 2),
        name="own_sums",
    )(matrix, *matched, *early, *chunks)


def cut_body(block, *outs):
    spd = outs[0].shape[0]
    for at, out in enumerate(outs):
        out[...] = block[pl.ds((at + 1) * spd, spd), :]


def cut(block, parts):
    spd, width = block.shape[0] // parts, block.shape[1]
    return pl.pallas_call(
        cut_body,
        out_shape=(jax.ShapeDtypeStruct((spd, width), block.dtype),) * (parts - 1),
        in_specs=[VM],
        out_specs=(VM,) * (parts - 1),
        compiler_params=room(2),
        cost_estimate=cost(block.size * 20, block.size * 4),
        name="cut",
    )(block)


PIECES = 4


def last_body(done, matrix, kept, far, same_chip, far_chip, cold, hot, held, sems, hot_held, hot_sem):
    table = matrix[...]
    size = ROWS // PIECES
    moves = []
    for piece in range(PIECES):
        where = pl.ds(piece * size, size)
        held[where, :] = done[where, :] + jnp.dot(far[where, :], table, preferred_element_type=jnp.float32)
        moves.append(pltpu.make_async_copy(held.at[where], cold.at[where], sems.at[piece]))
        moves[-1].start()
        if piece == 0:
            hot_far = far[pl.ds(ROWS, hot.shape[0]), :].astype(jnp.float32)
            hot_held[...] = kept[...] + same_chip[...] + project(hot_far + far_chip[...], table)
            moves.append(pltpu.make_async_copy(hot_held, hot, hot_sem))
            moves[-1].start()
    for one in moves:
        one.wait()


def last(done, matrix, kept, far, same_chip, far_chip):
    half, width = same_chip.shape
    return pl.pallas_call(
        last_body,
        out_shape=(
            jax.ShapeDtypeStruct((ROWS, width), jnp.float32),
            jax.ShapeDtypeStruct((half, width), jnp.float32),
        ),
        in_specs=[VM] * 6,
        out_specs=(HB, HB),
        scratch_shapes=[
            pltpu.VMEM((ROWS, width), jnp.float32),
            pltpu.SemaphoreType.DMA((PIECES,)),
            pltpu.VMEM((half, width), jnp.float32),
            pltpu.SemaphoreType.DMA,
        ],
        compiler_params=room(4),
        cost_estimate=cost(4 * ROWS * width * width, ROWS * width * 10),
        name="last",
    )(done, matrix, kept, far, same_chip, far_chip)


def swap_reps(block):
    reps = lax.axis_size("rep")
    return lax.ppermute(block, "rep", [(r, r ^ 1) for r in range(reps)])


FIRST = (7, 6, 5, 4, 3, 2, 1)
PLANE = (1, 2, 3)
SPLIT = ()
EARLY = (0, 4, 3, 7, 6, 5)


def shards(grad_out, indices, projections, widths, hot_ids):
    count, reps = lax.axis_size("tab"), lax.axis_size("rep")
    spd, tables, width = grad_out.shape
    half_len = count // 2 * spd
    hots = hot_ids.shape[1]
    grads = grad_out.reshape(spd, tables // SUB, SUB, width)

    def send(block, shift):
        return lax.ppermute(block, "tab", [(i, i ^ shift) for i in range(count)])

    notes, *blocks, relay = prep(grads, indices, hot_ids)
    got = {0: blocks[0]}
    for shift in FIRST:
        got[shift] = send(blocks[shift], shift)
    far_notes = send(notes, SUB)
    relayed = send(relay, SUB // 2)
    far_matched = match(far_notes, half_len, hots)
    far_early = early_sums(spd, far_matched, [(shift, 0, got[shift]) for shift in EARLY])
    partial, far_given = other_sums(
        spd, far_matched, far_early, [(shift, 0, got[shift]) for shift in range(SUB) if shift not in EARLY]
    )
    far = send(partial, SUB)
    own = [(shift, spd, got[shift]) for shift in (0,) + PLANE if shift not in SPLIT]
    own += [(shift, 0, send(block, shift)) for shift, block in zip(SPLIT, blocks[SUB:])]
    own += [(SUB // 2, 0, relayed)]
    pieces = cut(relayed, SUB // 2)
    second = [send(pieces[shift - 1], shift) for shift in PLANE]
    far_chip = lax.ppermute(
        far_given,
        ("rep", "tab"),
        [(r * count + i, (r ^ 1) * count + (i ^ SUB)) for r in range(reps) for i in range(count)],
    )
    own_matched = match(notes, half_len, hots)
    *own_early, matrix = early_sums(spd, own_matched, own, widths, projections[0])
    done, kept, given = own_sums(
        spd, own_matched, own_early, [(SUB // 2 + shift, 0, one) for shift, one in zip(PLANE, second)], matrix
    )
    same_chip = swap_reps(given)
    cold, hot = last(done, matrix, kept, far, same_chip, far_chip)
    return cold[None, None], hot[None]


def block_sums(narrow_rows, lookups):
    total_len = narrow_rows.shape[0]
    block_len = math.gcd(total_len, 4096)
    positions = lax.broadcasted_iota(jnp.int32, (1, ROWS), 1)

    def add_block(block, totals):
        piece_rows = lax.dynamic_slice_in_dim(narrow_rows, block * block_len, block_len, 0)
        row_ids = lax.dynamic_slice_in_dim(lookups, block * block_len, block_len, 0)
        onehot = (row_ids[:, None] == positions).astype(jnp.bfloat16)
        return totals + lax.dot_general(
            onehot, piece_rows, (((0,), (0,)), ((), ())), preferred_element_type=jnp.float32
        )

    start_sums = jnp.zeros((ROWS, narrow_rows.shape[1]), jnp.float32)
    return lax.fori_loop(0, total_len // block_len, add_block, start_sums)


def many_shards(grad_out, indices, projections, widths, hot_ids):
    columns = lax.broadcasted_iota(jnp.int32, (1, projections.shape[2]), 1)
    limit = lax.dynamic_slice_in_dim(widths, lax.axis_index("tab"), 1, 0)
    received = lax.all_to_all(grad_out, "tab", split_axis=1, concat_axis=0, tiled=True)
    full_proj = jnp.einsum("be,ej->bj", received[:, 0], projections[0], preferred_element_type=jnp.float32)
    narrow = jnp.where(columns < limit[:, None], full_proj, 0.0).astype(jnp.bfloat16)
    row_grads = block_sums(narrow, indices[0])
    own_hot = row_grads[hot_ids[0]]
    half_hot = own_hot.shape[0] // 2
    replica = lax.axis_index("rep")
    kept_rows = lax.dynamic_slice_in_dim(own_hot, replica * half_hot, half_hot, 0)
    given_rows = lax.dynamic_slice_in_dim(own_hot, (1 - replica) * half_hot, half_hot, 0)
    hot_grad = kept_rows + swap_reps(given_rows)
    all_rows = lax.broadcasted_iota(jnp.int32, (ROWS, 1), 0)
    is_hot = jnp.any(hot_ids == all_rows, axis=1)
    cold_grad = jnp.where(is_hot[:, None], jnp.float32(0.0), row_grads)
    return cold_grad[None, None], hot_grad[None]


def solution(mesh):
    placed = (
        P(("rep", "tab"), None, None),
        P("tab", "rep"),
        P("tab", None, None),
        P(),
        P("tab", None),
    )
    few = mesh.shape["tab"] <= MOST_PEERS
    return jax.shard_map(
        shards if few else many_shards,
        mesh=mesh,
        in_specs=placed,
        out_specs=(P("rep", "tab", None, None), P("tab", "rep", None)),
        check_vma=False,
    )
```
